256 devices in a mesh: seq: 32 (over x, z), head: 8 (over y, core).
Axes of the slice: x: 4, y: 4, z: 8, core: 2. Of those that a mesh axis runs over, the one named last changes fastest.
Arguments:
- queries: bfloat16 [32, 64, 128], P('seq', 'head'), may hold values from -90 to 90
- keys: bfloat16 [32, 8, 16384, 128], P(None, 'head', 'seq'), may hold values from -4 to 4
- values: bfloat16 [32, 8, 16384, 128], P(None, 'head', 'seq'), may hold values from -6 to 6
- old_scores: float32 [32, 8, 16384], P(None, 'head', 'seq'), may hold values from 0 to 4
- lengths: int32 [32], replicated, may hold values from 4096 to 16384
- valid_counts: int32 [32, 128], P(None, 'seq'), may hold values from 1 to 128
Outputs:
- attended: bfloat16 [32, 64, 128], P('seq', 'head')
- heavy_scores: float32 [32, 8, 16384], P(None, 'head', 'seq')
The draws below stay inside these ranges and needn't reach their ends.
Inputs may be any that keep to these rules, and one draw needn't show every extreme that they name: `lengths`: slot c of a sequence is cached when c is below its length. `valid_counts`: in block k of a sequence, the slots k * 128 + j with j below the count are live and the others are evicted.
All inputs are finite; a program needn't handle non-finite values.
Results may differ from the reference program's by a relative error of at most 0.0075.
Values may be sent and summed in bfloat16 or wider, within the bound.
A program may use at most 64 MiB of HBM per device.

```python
import jax
import jax.numpy as jnp
from jax import lax

QH = 64
KVH = 8
HD = 128
BLK = 128
SEQS = 32
CTX = 16384
NBLK = 128


def anchor_rows(key):
    return jnp.clip(jax.random.normal(jax.random.fold_in(key, 13), (SEQS, KVH, HD), jnp.float32), -4.0, 4.0)


def draw_keys(key, part):
    bulk = jnp.clip(jax.random.normal(jax.random.fold_in(key, 12), (SEQS, KVH, CTX, HD), jnp.float32), -4.0, 4.0)
    anchor = anchor_rows(key)
    bulk = bulk.at[:, :, 0, :].set(anchor)
    return bulk.astype(jnp.bfloat16)


def draw_queries(key, part):
    bulk = jnp.clip(jax.random.normal(jax.random.fold_in(key, 11), (SEQS, QH, HD), jnp.float32), -4.0, 4.0)
    log_scale = jax.random.uniform(jax.random.fold_in(key, 14), (SEQS, QH, 1), jnp.float32, 0.0, jnp.log(4.0))
    bulk = bulk * jnp.exp(log_scale)
    return bulk.astype(jnp.bfloat16)


def touch_ends(values, own_key, low, top_value):
    index_at = [jax.random.randint(jax.random.fold_in(own_key, axis), (), 0, length) for axis, length in enumerate(values.shape)]
    widest = values.shape.index(max(values.shape))
    next_to = index_at[:widest] + [(index_at[widest] + 1) % values.shape[widest]] + index_at[widest + 1:]
    return values.at[tuple(index_at)].set(low).at[tuple(next_to)].set(top_value)


def level_of(stream_key, extent, pieces, least, high):
    gain, own = 1.0, jax.random.fold_in(stream_key, 6)
    for dim, blocks in pieces:
        heights = jnp.exp(jax.random.uniform(jax.random.fold_in(own, dim), (blocks,), jnp.float32, least / len(pieces), high / len(pieces)))
        gain = gain * jnp.repeat(heights, extent[dim] // blocks).reshape([-1 if axis == dim else 1 for axis in range(len(extent))])
    return gain


def centred(rng, shape, scale, limit, shards=(), held_as=jnp.bfloat16):
    result = scale * jax.random.normal(rng, shape, jnp.float32)
    if shards:
        result = result * level_of(rng, shape, shards, -0.22, 0.18)
    return jnp.clip(result, -limit, limit).astype(held_as)


def setup_inputs(seed: int = 0) -> dict:
    splits = jax.random.split(jax.random.key(seed), 7)
    queries = draw_queries(jax.random.fold_in(splits[6], 71), 0)
    keys = draw_keys(jax.random.fold_in(splits[6], 71), 0)
    values = centred(splits[2], (SEQS, KVH, CTX, HD), 1.0, 6.0, ((1, 8), (2, 32)))
    old_scores = jnp.clip(4.0 * jax.random.uniform(splits[3], (SEQS, KVH, CTX), jnp.float32) ** level_of(splits[3], (SEQS, KVH, CTX), ((1, 8), (2, 32)), -0.2, 0.2), 0.0, 4.0)
    lengths = touch_ends(jax.random.randint(splits[4], (SEQS,), CTX // 4, CTX + 1), jax.random.fold_in(splits[4], 1), CTX // 4, CTX).astype(jnp.int32)
    valid_counts = touch_ends(jax.random.randint(splits[5], (SEQS, NBLK), 1, BLK + 1), jax.random.fold_in(splits[5], 1), 1, BLK).astype(jnp.int32)
    return dict(queries=queries, keys=keys, values=values, old_scores=old_scores, lengths=lengths, valid_counts=valid_counts)


def one_sequence(sequence_item):
    query_rows, key_rows, value_rows, old_rows, length, counts = sequence_item
    group_size = QH // KVH
    grouped = query_rows.astype(jnp.float32).reshape(KVH, group_size, HD)
    scores = jnp.einsum("hgd,hcd->hgc", grouped, key_rows.astype(jnp.float32)) * (HD ** -0.5)
    position = jnp.arange(CTX, dtype=jnp.int32)
    live_mask = (position < length) & ((position % BLK) < jnp.repeat(counts, BLK))
    masked = jnp.where(live_mask[None, None, :], scores, -jnp.inf)
    row_top = jnp.max(masked, axis=2, keepdims=True)
    exponent = jnp.exp(masked - row_top)
    row_total = jnp.sum(exponent, axis=2, keepdims=True)
    weights = lax.optimization_barrier(exponent.astype(jnp.bfloat16))
    mixed_rows = jnp.einsum("hgc,hcd->hgd", weights.astype(jnp.float32), value_rows.astype(jnp.float32))
    attended = (mixed_rows / row_total).astype(jnp.bfloat16).reshape(QH, HD)
    heavy_rows = old_rows + jnp.sum(exponent / row_total, axis=1)
    return attended, heavy_rows


def reference(queries, keys, values, old_scores, lengths, valid_counts):
    attended, heavy_scores = lax.map(one_sequence, (queries, keys, values, old_scores, lengths, valid_counts))
    return attended, heavy_scores
```

```python
import functools

import jax
import jax.numpy as jnp
from jax import lax
from jax.experimental import pallas as pl
from jax.experimental.pallas import tpu as pltpu
from jax.sharding import PartitionSpec as P

HD = 128
BLK = 128
NX, NZ = 4, 8
NEG = -1e30
FLOOR = -1e29
TINY = 1e-30
MESH = pl.DeviceIdType.MESH


def zigzag(k):
    return ((k + 1) // 2) * (2 * (k % 2) - 1)


def kernel(
    n, heads, ctx, q_hbm, k_hbm, v_hbm, len_hbm, val_hbm, con_ref, att_ref,
    kbuf, vbuf, qbuf, obuf, mixbuf, pbuf, stat, statall, ltot, len_s, val_s,
    ksem, vsem, lsem, qsend, qrecv, osend, orecv, ssend, srecv,
):
    me = lax.axis_index("seq")
    mx, mz = me // NZ, me % NZ
    blocks = ctx // BLK
    half = n // 2

    def peer_at(i):
        dx = NX // 2 + zigzag(i % NX)
        dz = NZ // 2 + zigzag(i // NX)
        return ((mx + dx) % NX) * NZ + (mz + dz) % NZ

    barrier = pltpu.get_barrier_semaphore()

    def greet(i, _):
        pl.semaphore_signal(barrier, inc=1, device_id={"seq": peer_at(i)}, device_id_type=MESH)
        return 0

    lax.fori_loop(0, n - 1, greet, 0, unroll=True)

    q_load = pltpu.make_async_copy(q_hbm.at[0], qbuf.at[me], lsem.at[0])
    len_load = pltpu.make_async_copy(len_hbm, len_s, lsem.at[1])
    val_load = pltpu.make_async_copy(val_hbm, val_s, lsem.at[2])
    q_load.start()
    len_load.start()
    val_load.start()
    loads = []
    for c in range(4):
        rows = pl.ds(c * (n // 4), n // 4)
        loads.append(pltpu.make_async_copy(k_hbm.at[rows, 0], kbuf.at[rows], ksem.at[c]))
        loads.append(pltpu.make_async_copy(v_hbm.at[rows, 0], vbuf.at[rows], vsem.at[c]))
    for load in loads:
        load.start()
    q_load.wait()
    pl.semaphore_wait(barrier, n - 1)

    def q_copy(slot, peer):
        return pltpu.make_async_remote_copy(
            src_ref=qbuf.at[me], dst_ref=qbuf.at[slot], send_sem=qsend.at[peer], recv_sem=qrecv.at[slot],
            device_id={"seq": peer}, device_id_type=MESH,
        )

    def o_copy(b, slot):
        return pltpu.make_async_remote_copy(
            src_ref=obuf.at[b], dst_ref=mixbuf.at[slot], send_sem=osend.at[b], recv_sem=orecv.at[slot],
            device_id={"seq": b}, device_id_type=MESH,
        )

    def s_copy(slot, peer):
        return pltpu.make_async_remote_copy(
            src_ref=stat, dst_ref=statall.at[slot], send_sem=ssend.at[peer], recv_sem=srecv.at[slot],
            device_id={"seq": peer}, device_id_type=MESH,
        )

    def send_q(i, _):
        q_copy(me, peer_at(i)).start()
        return 0

    lax.fori_loop(0, n - 1, send_q, 0, unroll=True)
    len_load.wait()
    val_load.wait()
    for load in loads:
        load.wait()

    base = me * ctx
    row2 = lax.broadcasted_iota(jnp.int32, (2 * heads, BLK), 0)
    lane2 = lax.broadcasted_iota(jnp.int32, (2 * heads, BLK), 1)
    upper = row2 < heads
    skew = (
        lax.broadcasted_iota(jnp.int32, (heads, BLK), 1)
        - lax.broadcasted_iota(jnp.int32, (heads, BLK), 0)
    )

    def scores_of(pair):
        b0 = 2 * pair
        qp = qbuf[pl.ds(b0, 2)].astype(jnp.float32).reshape(2 * heads, HD)
        lhs = jnp.concatenate([jnp.where(upper, qp, 0.0), jnp.where(upper, 0.0, qp)], axis=1).astype(jnp.bfloat16)
        keys = jnp.concatenate([kbuf[b0], kbuf[b0 + 1]], axis=1)
        s = lax.dot_general(lhs, keys, (((1,), (1,)), ((), ())), preferred_element_type=jnp.float32)
        s = s * HD ** (-0.5)
        parts = []
        for j in range(blocks):
            lim = [jnp.minimum(val_s[j, b0 + r], len_s[b0 + r] - base - j * BLK) for r in range(2)]
            limit = jnp.where(upper, lim[0], lim[1])
            parts.append(jnp.where(lane2 < limit, s[:, j * BLK : (j + 1) * BLK], NEG))
        return parts

    def tree(op, parts):
        while len(parts) > 1:
            parts = [op(parts[i], parts[i + 1]) for i in range(0, len(parts), 2)]
        return parts[0]

    def group(gi, carry):
        l0, l1, m0, m1 = carry
        zo = (mz // 2 + zigzag(gi)) % (NZ // 2)
        pairs = [((mx + xo) % NX) * (NZ // 2) + zo for xo in (0, 1, 3, 2)]
        for pair in pairs:
            for r in range(2):
                b = 2 * pair + r

                @pl.when(b != me)
                def _():
                    q_copy(b, b).wait_recv()

        parts = [scores_of(pair) for pair in pairs]
        tops = [
            jnp.maximum(jnp.max(tree(jnp.maximum, ps), axis=1, keepdims=True), FLOOR) for ps in parts
        ]
        expos = [[jnp.exp(s - top) for s in ps] for ps, top in zip(parts, tops)]
        totals = [
            jnp.maximum(jnp.sum(tree(jnp.add, es), axis=1, keepdims=True), TINY) for es in expos
        ]
        for pair, top, es, total in zip(pairs, tops, expos, totals):
            b0 = 2 * pair
            w = jnp.concatenate(es, axis=1).astype(jnp.bfloat16)
            pbuf[pl.ds(pl.multiple_of(pair * 2 * heads, 2 * heads), 2 * heads), :] = w
            vals = jnp.concatenate([vbuf[b0], vbuf[b0 + 1]], axis=1)
            mixed = jnp.dot(w, vals, preferred_element_type=jnp.float32)
            inv = 1.0 / total
            lse = top + jnp.log(total)
            for r in range(2):
                rows = slice(r * heads, (r + 1) * heads)
                part = mixed[rows, r * HD : (r + 1) * HD] * inv[rows]
                obuf[b0 + r] = part.astype(jnp.bfloat16)
                at = (b0 + r) * heads
                l0 = jnp.where(skew == at, lse[rows], l0)
                l1 = jnp.where(skew == at - BLK, lse[rows], l1)
                m0 = jnp.where(skew == at, top[rows], m0)
                m1 = jnp.where(skew == at - BLK, top[rows], m1)
        for pair in pairs:
            for r in range(2):
                b = 2 * pair + r

                @pl.when(b != me)
                def _():
                    o_copy(b, me).start()

        return l0, l1, m0, m1

    zero = jnp.zeros((heads, BLK), jnp.float32)
    l0, l1, m0, m1 = lax.fori_loop(0, NZ // 2, group, (zero, zero, zero, zero))

    own = jnp.concatenate([jnp.sum(l0, axis=0, keepdims=True), jnp.sum(l1, axis=0, keepdims=True)], axis=0)
    tops = jnp.concatenate([jnp.sum(m0, axis=0, keepdims=True), jnp.sum(m1, axis=0, keepdims=True)], axis=0)
    stat[...] = own
    statall[me] = own

    def send_s(i, _):
        s_copy(me, peer_at(i)).start()
        return 0

    lax.fori_loop(0, n - 1, send_s, 0, unroll=True)
    mixbuf[me] = obuf[me]

    def take_s(i, _):
        src = peer_at(n - 2 - i)
        s_copy(src, src).wait_recv()
        return 0

    lax.fori_loop(0, n - 1, take_s, 0, unroll=True)

    every = statall[...]
    top = jnp.max(every, axis=0)
    lse = top + jnp.log(jnp.sum(jnp.exp(every - top[None]), axis=0))
    ltot[...] = lse
    share = jnp.exp(tops - lse)
    rows_h = lax.broadcasted_iota(jnp.int32, (half, BLK), 0)
    lanes_h = lax.broadcasted_iota(jnp.int32, (half, BLK), 1) // heads
    for r in range(2):
        spread = jnp.where(rows_h == lanes_h, jnp.broadcast_to(share[r : r + 1], (half, BLK)), 0.0)
        high = spread.astype(jnp.bfloat16)
        low = (spread - high.astype(jnp.float32)).astype(jnp.bfloat16)
        both = jnp.concatenate([high, low], axis=0)
        got = jnp.dot(both, pbuf[r * BLK : (r + 1) * BLK, :], preferred_element_type=jnp.float32)
        con_ref[r * half : (r + 1) * half, :] = got[:half] + got[half:]

    def take_o(i, _):
        src = peer_at(n - 2 - i)
        o_copy(src, src).wait_recv()
        return 0

    lax.fori_loop(0, n - 1, take_o, 0, unroll=True)

    my_row = me // half
    hit = skew == (me % half) * heads
    total_row = ltot[pl.ds(my_row, 1), :]
    acc = zero
    for d in range(n):
        gap = jnp.broadcast_to(statall[d, pl.ds(my_row, 1), :] - total_row, (heads, BLK))
        part = jnp.exp(jnp.sum(jnp.where(hit, gap, 0.0), axis=1, keepdims=True))
        acc = acc + part * mixbuf[d].astype(jnp.float32)
    att_ref[...] = acc

    def finish(i, _):
        peer = peer_at(i)
        q_copy(me, peer).wait_send()
        o_copy(peer, me).wait_send()
        s_copy(me, peer).wait_send()
        return 0

    lax.fori_loop(0, n - 1, finish, 0, unroll=True)


def on_device(queries, keys, values, old_scores, lengths, valid_counts):
    n = lax.axis_size("seq")
    heads = queries.shape[1]
    ctx = keys.shape[2]
    blocks = ctx // BLK
    anywhere = pl.BlockSpec(memory_space=pl.ANY)
    vmem = pl.BlockSpec(memory_space=pltpu.VMEM)
    dma = pltpu.SemaphoreType.DMA
    added, attended = pl.pallas_call(
        functools.partial(kernel, n, heads, ctx),
        out_shape=(
            jax.ShapeDtypeStruct((n, ctx), jnp.float32),
            jax.ShapeDtypeStruct((heads, HD), jnp.float32),
        ),
        in_specs=[anywhere] * 5,
        out_specs=(vmem, vmem),
        scratch_shapes=[
            pltpu.VMEM((n, ctx, HD), jnp.bfloat16),
            pltpu.VMEM((n, ctx, HD), jnp.bfloat16),
            pltpu.VMEM((n, heads, HD), jnp.bfloat16),
            pltpu.VMEM((n, heads, HD), jnp.bfloat16),
            pltpu.VMEM((n, heads, HD), jnp.bfloat16),
            pltpu.VMEM((n * heads, ctx), jnp.bfloat16),
            pltpu.VMEM((2, BLK), jnp.float32),
            pltpu.VMEM((n, 2, BLK), jnp.float32),
            pltpu.VMEM((2, BLK), jnp.float32),
            pltpu.SMEM((n,), jnp.int32),
            pltpu.SMEM((blocks, n), jnp.int32),
            dma((4,)),
            dma((4,)),
            dma((3,)),
            dma((n,)),
            dma((n,)),
            dma((n,)),
            dma((n,)),
            dma((n,)),
            dma((n,)),
        ],
        compiler_params=pltpu.CompilerParams(collective_id=0, has_side_effects=True),
        name="decode",
    )(queries, keys, values, lengths, valid_counts.T)
    heavy = old_scores + added.reshape(old_scores.shape)
    return attended.astype(jnp.bfloat16)[None], heavy


def solution(mesh):
    return jax.shard_map(
        on_device,
        mesh=mesh,
        in_specs=(
            P("seq", "head", None),
            P(None, "head", "seq", None),
            P(None, "head", "seq", None),
            P(None, "head", "seq"),
            P(),
            P(None, "seq"),
        ),
        out_specs=(P("seq", "head", None), P(None, "head", "seq")),
        check_vma=False,
    )
```

```python
import functools

import jax
import jax.numpy as jnp
from jax import lax
from jax.experimental import pallas as pl
from jax.experimental.pallas import tpu as pltpu
from jax.sharding import PartitionSpec as P

HD = 128
BLK = 128
NX, NZ = 4, 8
NEG = -1e30
FLOOR = -1e29
TINY = 1e-30
MESH = pl.DeviceIdType.MESH


def zigzag(k):
    return ((k + 1) // 2) * (2 * (k % 2) - 1)


def kernel(
    n, heads, ctx, q_hbm, k_hbm, v_hbm, len_hbm, val_hbm, con_ref, att_ref,
    kbuf, vbuf, kturn, qbuf, obuf, mixbuf, pbuf, stat, statall, ltot, len_s, val_s,
    ksem, vsem, lsem, qsend, qrecv, osend, orecv, ssend, srecv,
):
    me = lax.axis_index("seq")
    mx, mz = me // NZ, me % NZ
    blocks = ctx // BLK
    half = n // 2

    def peer_at(i):
        dx = NX // 2 + zigzag(i % NX)
        dz = NZ // 2 + zigzag(i // NX)
        return ((mx + dx) % NX) * NZ + (mz + dz) % NZ

    barrier = pltpu.get_barrier_semaphore()

    def greet(i, _):
        pl.semaphore_signal(barrier, inc=1, device_id={"seq": peer_at(i)}, device_id_type=MESH)
        return 0

    lax.fori_loop(0, n - 1, greet, 0, unroll=True)

    q_load = pltpu.make_async_copy(q_hbm.at[0], qbuf.at[me], lsem.at[0])
    len_load = pltpu.make_async_copy(len_hbm, len_s, lsem.at[1])
    val_load = pltpu.make_async_copy(val_hbm, val_s, lsem.at[2])
    q_load.start()
    len_load.start()
    val_load.start()
    loads = []
    for c in range(4):
        rows = pl.ds(c * (n // 4), n // 4)
        loads.append(pltpu.make_async_copy(k_hbm.at[rows, 0], kbuf.at[rows], ksem.at[c]))
        loads.append(pltpu.make_async_copy(v_hbm.at[rows, 0], vbuf.at[rows], vsem.at[c]))
    for load in loads:
        load.start()
    q_load.wait()
    pl.semaphore_wait(barrier, n - 1)

    def q_copy(slot, peer):
        return pltpu.make_async_remote_copy(
            src_ref=qbuf.at[me], dst_ref=qbuf.at[slot], send_sem=qsend.at[peer], recv_sem=qrecv.at[slot],
            device_id={"seq": peer}, device_id_type=MESH,
        )

    def o_copy(b, slot):
        return pltpu.make_async_remote_copy(
            src_ref=obuf.at[b], dst_ref=mixbuf.at[slot], send_sem=osend.at[b], recv_sem=orecv.at[slot],
            device_id={"seq": b}, device_id_type=MESH,
        )

    def s_copy(slot, peer):
        return pltpu.make_async_remote_copy(
            src_ref=stat, dst_ref=statall.at[slot], send_sem=ssend.at[peer], recv_sem=srecv.at[slot],
            device_id={"seq": peer}, device_id_type=MESH,
        )

    def send_q(i, _):
        q_copy(me, peer_at(i)).start()
        return 0

    lax.fori_loop(0, n - 1, send_q, 0, unroll=True)
    len_load.wait()
    val_load.wait()
    for load in loads:
        load.wait()

    def turn(b, _):
        kturn[b] = kbuf[b].T
        return 0

    lax.fori_loop(0, n, turn, 0, unroll=4)

    base = me * ctx
    row2 = lax.broadcasted_iota(jnp.int32, (2 * heads, BLK), 0)
    lane2 = lax.broadcasted_iota(jnp.int32, (2 * heads, BLK), 1)
    upper = row2 < heads
    skew = (
        lax.broadcasted_iota(jnp.int32, (heads, BLK), 1)
        - lax.broadcasted_iota(jnp.int32, (heads, BLK), 0)
    )

    def scores_of(pair):
        b0 = 2 * pair
        qp = qbuf[pl.ds(b0, 2)].astype(jnp.float32).reshape(2 * heads, HD)
        lhs = jnp.concatenate([jnp.where(upper, qp, 0.0), jnp.where(upper, 0.0, qp)], axis=1).astype(jnp.bfloat16)
        keys = jnp.concatenate([kturn[b0], kturn[b0 + 1]], axis=0)
        s = jnp.dot(lhs, keys, preferred_element_type=jnp.float32)
        s = s * HD ** (-0.5)
        parts = []
        for j in range(blocks):
            lim = [jnp.minimum(val_s[j, b0 + r], len_s[b0 + r] - base - j * BLK) for r in range(2)]
            limit = jnp.where(upper, lim[0], lim[1])
            parts.append(jnp.where(lane2 < limit, s[:, j * BLK : (j + 1) * BLK], NEG))
        return parts

    def tree(op, parts):
        while len(parts) > 1:
            parts = [op(parts[i], parts[i + 1]) for i in range(0, len(parts), 2)]
        return parts[0]

    def group(gi, carry):
        l0, l1, m0, m1 = carry
        zo = (mz // 2 + zigzag(gi)) % (NZ // 2)
        pairs = [((mx + xo) % NX) * (NZ // 2) + zo for xo in (0, 1, 3, 2)]
        for pair in pairs:
            for r in range(2):
                b = 2 * pair + r

                @pl.when(b != me)
                def _():
                    q_copy(b, b).wait_recv()

        parts = [scores_of(pair) for pair in pairs]
        tops = [
            jnp.maximum(jnp.max(tree(jnp.maximum, ps), axis=1, keepdims=True), FLOOR) for ps in parts
        ]
        expos = [[jnp.exp(s - top) for s in ps] for ps, top in zip(parts, tops)]
        totals = [
            jnp.maximum(jnp.sum(tree(jnp.add, es), axis=1, keepdims=True), TINY) for es in expos
        ]
        for pair, top, es, total in zip(pairs, tops, expos, totals):
            b0 = 2 * pair
            w = jnp.concatenate(es, axis=1).astype(jnp.bfloat16)
            pbuf[pl.ds(pl.multiple_of(pair * 2 * heads, 2 * heads), 2 * heads), :] = w
            vals = jnp.concatenate([vbuf[b0], vbuf[b0 + 1]], axis=1)
            mixed = jnp.dot(w, vals, preferred_element_type=jnp.float32)
            inv = 1.0 / total
            lse = top + jnp.log(total)
            for r in range(2):
                rows = slice(r * heads, (r + 1) * heads)
                part = mixed[rows, r * HD : (r + 1) * HD] * inv[rows]
                obuf[b0 + r] = part.astype(jnp.bfloat16)
                at = (b0 + r) * heads
                l0 = jnp.where(skew == at, lse[rows], l0)
                l1 = jnp.where(skew == at - BLK, lse[rows], l1)
                m0 = jnp.where(skew == at, top[rows], m0)
                m1 = jnp.where(skew == at - BLK, top[rows], m1)
        for pair in pairs:
            for r in range(2):
                b = 2 * pair + r

                @pl.when(b != me)
                def _():
                    o_copy(b, me).start()

        return l0, l1, m0, m1

    zero = jnp.zeros((heads, BLK), jnp.float32)
    l0, l1, m0, m1 = lax.fori_loop(0, NZ // 2, group, (zero, zero, zero, zero))

    own = jnp.concatenate([jnp.sum(l0, axis=0, keepdims=True), jnp.sum(l1, axis=0, keepdims=True)], axis=0)
    tops = jnp.concatenate([jnp.sum(m0, axis=0, keepdims=True), jnp.sum(m1, axis=0, keepdims=True)], axis=0)
    stat[...] = own
    statall[me] = own

    def send_s(i, _):
        s_copy(me, peer_at(i)).start()
        return 0

    lax.fori_loop(0, n - 1, send_s, 0, unroll=True)
    mixbuf[me] = obuf[me]

    def take_s(i, _):
        src = peer_at(n - 2 - i)
        s_copy(src, src).wait_recv()
        return 0

    lax.fori_loop(0, n - 1, take_s, 0, unroll=True)

    every = statall[...]
    top = jnp.max(every, axis=0)
    lse = top + jnp.log(jnp.sum(jnp.exp(every - top[None]), axis=0))
    ltot[...] = lse
    share = jnp.exp(tops - lse)
    rows_h = lax.broadcasted_iota(jnp.int32, (half, BLK), 0)
    lanes_h = lax.broadcasted_iota(jnp.int32, (half, BLK), 1) // heads
    for r in range(2):
        spread = jnp.where(rows_h == lanes_h, jnp.broadcast_to(share[r : r + 1], (half, BLK)), 0.0)
        high = spread.astype(jnp.bfloat16)
        low = (spread - high.astype(jnp.float32)).astype(jnp.bfloat16)
        both = jnp.concatenate([high, low], axis=0)
        got = jnp.dot(both, pbuf[r * BLK : (r + 1) * BLK, :], preferred_element_type=jnp.float32)
        got = got[:half] + got[half:]
        for j in range(blocks):
            con_ref[pl.ds(r * half * blocks + j, half, stride=blocks), :] = got[:, j * BLK : (j + 1) * BLK]

    def take_o(i, _):
        src = peer_at(n - 2 - i)
        o_copy(src, src).wait_recv()
        return 0

    lax.fori_loop(0, n - 1, take_o, 0, unroll=True)

    my_row = me // half
    hit = skew == (me % half) * heads
    total_row = ltot[pl.ds(my_row, 1), :]
    acc = zero
    for d in range(n):
        gap = jnp.broadcast_to(statall[d, pl.ds(my_row, 1), :] - total_row, (heads, BLK))
        part = jnp.exp(jnp.sum(jnp.where(hit, gap, 0.0), axis=1, keepdims=True))
        acc = acc + part * mixbuf[d].astype(jnp.float32)
    att_ref[...] = acc

    def finish(i, _):
        peer = peer_at(i)
        q_copy(me, peer).wait_send()
        o_copy(peer, me).wait_send()
        s_copy(me, peer).wait_send()
        return 0

    lax.fori_loop(0, n - 1, finish, 0, unroll=True)


def closing(con_ref, att_ref, old_ref, attended_ref, heavy_ref):
    attended_ref[...] = att_ref[...].astype(jnp.bfloat16)
    heavy_ref[...] = old_ref[...] + con_ref[...]


def on_device(queries, keys, values, old_scores, lengths, valid_counts):
    n = lax.axis_size("seq")
    heads = queries.shape[1]
    ctx = keys.shape[2]
    blocks = ctx // BLK
    anywhere = pl.BlockSpec(memory_space=pltpu.HBM)
    vmem = pl.BlockSpec(memory_space=pltpu.VMEM)
    dma = pltpu.SemaphoreType.DMA
    added, attended = pl.pallas_call(
        functools.partial(kernel, n, heads, ctx),
        out_shape=(
            jax.ShapeDtypeStruct((n * blocks, BLK), jnp.float32),
            jax.ShapeDtypeStruct((heads, HD), jnp.float32),
        ),
        in_specs=[anywhere] * 5,
        out_specs=(vmem, vmem),
        scratch_shapes=[
            pltpu.VMEM((n, ctx, HD), jnp.bfloat16),
            pltpu.VMEM((n, ctx, HD), jnp.bfloat16),
            pltpu.VMEM((n, HD, ctx), jnp.bfloat16),
            pltpu.VMEM((n, heads, HD), jnp.bfloat16),
            pltpu.VMEM((n, heads, HD), jnp.bfloat16),
            pltpu.VMEM((n, heads, HD), jnp.bfloat16),
            pltpu.VMEM((n * heads, ctx), jnp.bfloat16),
            pltpu.VMEM((2, BLK), jnp.float32),
            pltpu.VMEM((n, 2, BLK), jnp.float32),
            pltpu.VMEM((2, BLK), jnp.float32),
            pltpu.SMEM((n,), jnp.int32),
            pltpu.SMEM((blocks, n), jnp.int32),
            dma((4,)),
            dma((4,)),
            dma((3,)),
            dma((n,)),
            dma((n,)),
            dma((n,)),
            dma((n,)),
            dma((n,)),
            dma((n,)),
        ],
        compiler_params=pltpu.CompilerParams(
            collective_id=0, has_side_effects=True, vmem_limit_bytes=16 * 2**20
        ),
        name="decode",
    )(*(pltpu.with_memory_space_constraint(a, pltpu.HBM) for a in (queries, keys, values, lengths, valid_counts.T)))
    attended, heavy = pl.pallas_call(
        closing,
        out_shape=(
            jax.ShapeDtypeStruct((heads, HD), jnp.bfloat16),
            jax.ShapeDtypeStruct((n * blocks, BLK), jnp.float32),
        ),
        in_specs=[vmem] * 3,
        out_specs=(vmem, vmem),
        compiler_params=pltpu.CompilerParams(vmem_limit_bytes=2**20),
        name="closing",
    )(added, attended, old_scores.reshape(n * blocks, BLK))
    return attended[None], heavy.reshape(old_scores.shape)


def solution(mesh):
    return jax.shard_map(
        on_device,
        mesh=mesh,
        in_specs=(
            P("seq", "head", None),
            P(None, "head", "seq", None),
            P(None, "head", "seq", None),
            P(None, "head", "seq"),
            P(),
            P(None, "seq"),
        ),
        out_specs=(P("seq", "head", None), P(None, "head", "seq")),
        check_vma=False,
    )
```

```python
import functools

import jax
import jax.numpy as jnp
from jax import lax
from jax.experimental import pallas as pl
from jax.experimental.pallas import tpu as pltpu
from jax.sharding import PartitionSpec as P

HD = 128
BLK = 128
NX, NZ = 4, 8
NEG = -1e30
FLOOR = -1e29
TINY = 1e-30
MESH = pl.DeviceIdType.MESH


def zigzag(k):
    return ((k + 1) // 2) * (2 * (k % 2) - 1)


def kernel(
    n, heads, ctx, q_hbm, k_hbm, v_hbm, len_hbm, val_hbm, con_ref, att_ref,
    kbuf, vbuf, kturn, qbuf, obuf, mixbuf, pbuf, stat, statall, ltot, len_s, val_s,
    ksem, vsem, lsem, qsend, qrecv, osend, orecv, ssend, srecv,
):
    me = lax.axis_index("seq")
    mx, mz = me // NZ, me % NZ
    blocks = ctx // BLK
    half = n // 2

    def pairs_of(k):
        zo = (mz // 2 + zigzag(k)) % (NZ // 2)
        return [((mx + xo) % NX) * (NZ // 2) + zo for xo in (0, 1, 3, 2)]

    def peers_of(k):
        found = []
        for pair in pairs_of(k)[::-1]:
            found += [2 * pair, 2 * pair + 1]
        return found[:-2] + [me + 1 - 2 * (me % 2)] if k == 0 else found

    groups = NZ // 2
    far_first = list(range(groups))[::-1]
    seen_as = (0, 2, 1, 3)

    barrier = pltpu.get_barrier_semaphore()
    for k in far_first:
        for peer in peers_of(k):
            pl.semaphore_signal(barrier, inc=1, device_id={"seq": peer}, device_id_type=MESH)

    q_load = pltpu.make_async_copy(q_hbm.at[0], qbuf.at[me], lsem.at[0])
    len_load = pltpu.make_async_copy(len_hbm, len_s, lsem.at[1])
    val_load = pltpu.make_async_copy(val_hbm, val_s, lsem.at[2])
    q_load.start()
    len_load.start()
    val_load.start()
    loads = []
    for c in range(4):
        rows = pl.ds(c * (n // 4), n // 4)
        loads.append(pltpu.make_async_copy(k_hbm.at[rows, 0], kbuf.at[rows], ksem.at[c]))
        loads.append(pltpu.make_async_copy(v_hbm.at[rows, 0], vbuf.at[rows], vsem.at[c]))
    for load in loads:
        load.start()
    q_load.wait()
    pl.semaphore_wait(barrier, n - 1)

    def q_copy(peer, k):
        return pltpu.make_async_remote_copy(
            src_ref=qbuf.at[me], dst_ref=qbuf.at[me], send_sem=qsend, recv_sem=qrecv.at[seen_as[k]],
            device_id={"seq": peer}, device_id_type=MESH,
        )

    def o_copy(b):
        return pltpu.make_async_remote_copy(
            src_ref=obuf.at[b], dst_ref=mixbuf.at[me], send_sem=osend, recv_sem=orecv,
            device_id={"seq": b}, device_id_type=MESH,
        )

    def s_copy(peer):
        return pltpu.make_async_remote_copy(
            src_ref=stat, dst_ref=statall.at[me], send_sem=ssend, recv_sem=srecv,
            device_id={"seq": peer}, device_id_type=MESH,
        )

    def await_slots(buf, count, sem):
        some = buf.at[pl.ds(0, count)]
        pltpu.make_async_copy(some, some, sem).wait()

    for k in far_first:
        for peer in peers_of(k):
            q_copy(peer, k).start()
    len_load.wait()
    val_load.wait()
    for load in loads:
        load.wait()

    def turn(b, _):
        kturn[b] = kbuf[b].T
        return 0

    lax.fori_loop(0, n, turn, 0, unroll=4)

    base = me * ctx
    row2 = lax.broadcasted_iota(jnp.int32, (2 * heads, BLK), 0)
    lane2 = lax.broadcasted_iota(jnp.int32, (2 * heads, BLK), 1)
    upper = row2 < heads
    skew = (
        lax.broadcasted_iota(jnp.int32, (heads, BLK), 1)
        - lax.broadcasted_iota(jnp.int32, (heads, BLK), 0)
    )

    def scores_of(pair):
        b0 = 2 * pair
        qp = qbuf[pl.ds(b0, 2)].astype(jnp.float32).reshape(2 * heads, HD)
        lhs = jnp.concatenate([jnp.where(upper, qp, 0.0), jnp.where(upper, 0.0, qp)], axis=1).astype(jnp.bfloat16)
        keys = jnp.concatenate([kturn[b0], kturn[b0 + 1]], axis=0)
        s = jnp.dot(lhs, keys, preferred_element_type=jnp.float32)
        s = s * HD ** (-0.5)
        parts = []
        for j in range(blocks):
            lim = [jnp.minimum(val_s[j, b0 + r], len_s[b0 + r] - base - j * BLK) for r in range(2)]
            limit = jnp.where(upper, lim[0], lim[1])
            parts.append(jnp.where(lane2 < limit, s[:, j * BLK : (j + 1) * BLK], NEG))
        return parts

    def tree(op, parts):
        while len(parts) > 1:
            parts = [op(parts[i], parts[i + 1]) for i in range(0, len(parts), 2)]
        return parts[0]

    def group(k, carry):
        l0, l1, m0, m1 = carry
        pairs = pairs_of(k)
        await_slots(qbuf, len(peers_of(k)), qrecv.at[k])
        parts = [scores_of(pair) for pair in pairs]
        tops = [
            jnp.maximum(jnp.max(tree(jnp.maximum, ps), axis=1, keepdims=True), FLOOR) for ps in parts
        ]
        expos = [[jnp.exp(s - top) for s in ps] for ps, top in zip(parts, tops)]
        totals = [
            jnp.maximum(jnp.sum(tree(jnp.add, es), axis=1, keepdims=True), TINY) for es in expos
        ]
        for pair, top, es, total in zip(pairs, tops, expos, totals):
            b0 = 2 * pair
            w = jnp.concatenate(es, axis=1).astype(jnp.bfloat16)
            pbuf[pl.ds(pl.multiple_of(pair * 2 * heads, 2 * heads), 2 * heads), :] = w
            vals = jnp.concatenate([vbuf[b0], vbuf[b0 + 1]], axis=1)
            mixed = jnp.dot(w, vals, preferred_element_type=jnp.float32)
            inv = 1.0 / total
            lse = top + jnp.log(total)
            for r in range(2):
                rows = slice(r * heads, (r + 1) * heads)
                part = mixed[rows, r * HD : (r + 1) * HD] * inv[rows]
                obuf[b0 + r] = part.astype(jnp.bfloat16)
                at = (b0 + r) * heads
                l0 = jnp.where(skew == at, lse[rows], l0)
                l1 = jnp.where(skew == at - BLK, lse[rows], l1)
                m0 = jnp.where(skew == at, top[rows], m0)
                m1 = jnp.where(skew == at - BLK, top[rows], m1)
        return l0, l1, m0, m1

    zero = jnp.zeros((heads, BLK), jnp.float32)
    carry = (zero, zero, zero, zero)
    for k in range(groups):
        carry = group(k, carry)
        if k < groups - 1:
            for peer in peers_of(k):
                o_copy(peer).start()
    l0, l1, m0, m1 = carry

    own = jnp.concatenate([jnp.sum(l0, axis=0, keepdims=True), jnp.sum(l1, axis=0, keepdims=True)], axis=0)
    tops = jnp.concatenate([jnp.sum(m0, axis=0, keepdims=True), jnp.sum(m1, axis=0, keepdims=True)], axis=0)
    stat[...] = own
    statall[me] = own

    for k in far_first:
        for peer in peers_of(k):
            s_copy(peer).start()
            if k == groups - 1:
                o_copy(peer).start()
    mixbuf[me] = obuf[me]
    await_slots(statall, n - 1, srecv)

    every = statall[...]
    top = jnp.max(every, axis=0)
    lse = top + jnp.log(jnp.sum(jnp.exp(every - top[None]), axis=0))
    ltot[...] = lse
    share = jnp.exp(tops - lse)
    rows_h = lax.broadcasted_iota(jnp.int32, (half, BLK), 0)
    lanes_h = lax.broadcasted_iota(jnp.int32, (half, BLK), 1) // heads
    for r in range(2):
        spread = jnp.where(rows_h == lanes_h, jnp.broadcast_to(share[r : r + 1], (half, BLK)), 0.0)
        high = spread.astype(jnp.bfloat16)
        low = (spread - high.astype(jnp.float32)).astype(jnp.bfloat16)
        both = jnp.concatenate([high, low], axis=0)
        got = jnp.dot(both, pbuf[r * BLK : (r + 1) * BLK, :], preferred_element_type=jnp.float32)
        got = got[:half] + got[half:]
        for j in range(blocks):
            con_ref[pl.ds(r * half * blocks + j, half, stride=blocks), :] = got[:, j * BLK : (j + 1) * BLK]

    await_slots(mixbuf, n - 1, orecv)
    my_row = me // half
    hit = skew == (me % half) * heads
    total_row = ltot[pl.ds(my_row, 1), :]
    acc = zero
    for d in range(n):
        gap = jnp.broadcast_to(statall[d, pl.ds(my_row, 1), :] - total_row, (heads, BLK))
        part = jnp.exp(jnp.sum(jnp.where(hit, gap, 0.0), axis=1, keepdims=True))
        acc = acc + part * mixbuf[d].astype(jnp.float32)
    att_ref[...] = acc

    await_slots(qbuf, n - 1, qsend)
    await_slots(obuf, n - 1, osend)
    await_slots(statall, n - 1, ssend)


def closing(con_ref, att_ref, old_ref, attended_ref, heavy_ref):
    attended_ref[...] = att_ref[...].astype(jnp.bfloat16)
    heavy_ref[...] = old_ref[...] + con_ref[...]


def on_device(queries, keys, values, old_scores, lengths, valid_counts):
    n = lax.axis_size("seq")
    heads = queries.shape[1]
    ctx = keys.shape[2]
    blocks = ctx // BLK
    anywhere = pl.BlockSpec(memory_space=pltpu.HBM)
    vmem = pl.BlockSpec(memory_space=pltpu.VMEM)
    dma = pltpu.SemaphoreType.DMA
    added, attended = pl.pallas_call(
        functools.partial(kernel, n, heads, ctx),
        out_shape=(
            jax.ShapeDtypeStruct((n * blocks, BLK), jnp.float32),
            jax.ShapeDtypeStruct((heads, HD), jnp.float32),
        ),
        in_specs=[anywhere] * 5,
        out_specs=(vmem, vmem),
        scratch_shapes=[
            pltpu.VMEM((n, ctx, HD), jnp.bfloat16),
            pltpu.VMEM((n, ctx, HD), jnp.bfloat16),
            pltpu.VMEM((n, HD, ctx), jnp.bfloat16),
            pltpu.VMEM((n, heads, HD), jnp.bfloat16),
            pltpu.VMEM((n, heads, HD), jnp.bfloat16),
            pltpu.VMEM((n, heads, HD), jnp.bfloat16),
            pltpu.VMEM((n * heads, ctx), jnp.bfloat16),
            pltpu.VMEM((2, BLK), jnp.float32),
            pltpu.VMEM((n, 2, BLK), jnp.float32),
            pltpu.VMEM((2, BLK), jnp.float32),
            pltpu.SMEM((n,), jnp.int32),
            pltpu.SMEM((blocks, n), jnp.int32),
            dma((4,)),
            dma((4,)),
            dma((3,)),
            dma,
            dma((NZ // 2,)),
            dma,
            dma,
            dma,
            dma,
        ],
        compiler_params=pltpu.CompilerParams(
            collective_id=0, has_side_effects=True, vmem_limit_bytes=16 * 2**20
        ),
        name="decode",
    )(*(pltpu.with_memory_space_constraint(a, pltpu.HBM) for a in (queries, keys, values, lengths, valid_counts.T)))
    attended, heavy = pl.pallas_call(
        closing,
        out_shape=(
            jax.ShapeDtypeStruct((heads, HD), jnp.bfloat16),
            jax.ShapeDtypeStruct((n * blocks, BLK), jnp.float32),
        ),
        in_specs=[vmem] * 3,
        out_specs=(vmem, vmem),
        compiler_params=pltpu.CompilerParams(vmem_limit_bytes=2**20),
        name="closing",
    )(added, attended, old_scores.reshape(n * blocks, BLK))
    return attended[None], heavy.reshape(old_scores.shape)


def solution(mesh):
    return jax.shard_map(
        on_device,
        mesh=mesh,
        in_specs=(
            P("seq", "head", None),
            P(None, "head", "seq", None),
            P(None, "head", "seq", None),
            P(None, "head", "seq"),
            P(),
            P(None, "seq"),
        ),
        out_specs=(P("seq", "head", None), P(None, "head", "seq")),
        check_vma=False,
    )
```

```python
import functools

import jax
import jax.numpy as jnp
from jax import lax
from jax.experimental import pallas as pl
from jax.experimental.pallas import tpu as pltpu
from jax.sharding import PartitionSpec as P

HD = 128
BLK = 128
NX, NZ = 4, 8
NEG = -1e30
FLOOR = -1e29
TINY = 1e-30
MESH = pl.DeviceIdType.MESH


def zigzag(k):
    return ((k + 1) // 2) * (2 * (k % 2) - 1)


def kernel(
    n, heads, ctx, q_hbm, k_hbm, v_hbm, old_hbm, len_hbm, val_hbm, new_ref, att_ref,
    kvbuf, old_v, kturn, qbuf, obuf, mixbuf, pbuf, ibuf, stat, statall, ltot, len_s, val_s,
    kvsem, lsem, osem, qrecv, orecv, ssend, srecv,
):
    me = lax.axis_index("seq")
    mx, mz = me // NZ, me % NZ
    blocks = ctx // BLK
    half = n // 2

    def pairs_of(k):
        zo = (mz // 2 + zigzag(k)) % (NZ // 2)
        return [((mx + xo) % NX) * (NZ // 2) + zo for xo in (0, 1, 3, 2)]

    def peers_of(k):
        found = []
        for pair in pairs_of(k)[::-1]:
            found += [2 * pair, 2 * pair + 1]
        return found[:-2] + [me + 1 - 2 * (me % 2)] if k == 0 else found

    groups = NZ // 2
    far_first = list(range(groups))[::-1]
    seen_as = (0, 2, 1, 3)

    barrier = pltpu.get_barrier_semaphore()
    for k in far_first:
        for peer in peers_of(k):
            pl.semaphore_signal(barrier, inc=1, device_id={"seq": peer}, device_id_type=MESH)

    q_load = pltpu.make_async_copy(q_hbm.at[0], qbuf.at[me], lsem.at[0])
    len_load = pltpu.make_async_copy(len_hbm, len_s, lsem.at[1])
    val_load = pltpu.make_async_copy(val_hbm, val_s, lsem.at[2])
    q_load.start()
    len_load.start()
    val_load.start()
    kbuf, vbuf = kvbuf.at[0], kvbuf.at[1]
    loads = [pltpu.make_async_copy(old_hbm, old_v, lsem.at[3])]
    for c in range(4):
        rows = pl.ds(c * (n // 4), n // 4)
        loads.append(pltpu.make_async_copy(k_hbm.at[rows, 0], kbuf.at[rows], kvsem))
        loads.append(pltpu.make_async_copy(v_hbm.at[rows, 0], vbuf.at[rows], kvsem))
    for load in loads:
        load.start()
    q_load.wait()
    pl.semaphore_wait(barrier, n - 1)

    def q_copy(peer, k):
        return pltpu.make_async_remote_copy(
            src_ref=qbuf.at[me], dst_ref=qbuf.at[me], send_sem=osem, recv_sem=qrecv.at[seen_as[k]],
            device_id={"seq": peer}, device_id_type=MESH,
        )

    def o_copy(b):
        return pltpu.make_async_remote_copy(
            src_ref=obuf.at[b], dst_ref=mixbuf.at[me], send_sem=osem, recv_sem=orecv,
            device_id={"seq": b}, device_id_type=MESH,
        )

    def s_copy(peer):
        return pltpu.make_async_remote_copy(
            src_ref=stat, dst_ref=statall.at[me], send_sem=ssend, recv_sem=srecv,
            device_id={"seq": peer}, device_id_type=MESH,
        )

    def await_slots(buf, count, sem):
        some = buf.at[pl.ds(0, count)]
        pltpu.make_async_copy(some, some, sem).wait()

    for k in far_first:
        for peer in peers_of(k):
            q_copy(peer, k).start()
    len_load.wait()
    val_load.wait()
    loads[0].wait()
    pltpu.make_async_copy(kvbuf, kvbuf, kvsem).wait()

    def turn(b, _):
        kturn[b] = kbuf[b].T
        return 0

    lax.fori_loop(0, n, turn, 0, unroll=4)

    base = me * ctx
    row2 = lax.broadcasted_iota(jnp.int32, (2 * heads, BLK), 0)
    lane2 = lax.broadcasted_iota(jnp.int32, (2 * heads, BLK), 1)
    upper = row2 < heads
    skew = (
        lax.broadcasted_iota(jnp.int32, (heads, BLK), 1)
        - lax.broadcasted_iota(jnp.int32, (heads, BLK), 0)
    )

    def product_of(pair):
        b0 = 2 * pair
        qp = qbuf[pl.ds(b0, 2)].astype(jnp.float32).reshape(2 * heads, HD)
        lhs = jnp.concatenate([jnp.where(upper, qp, 0.0), jnp.where(upper, 0.0, qp)], axis=1).astype(jnp.bfloat16)
        keys = jnp.concatenate([kturn[b0], kturn[b0 + 1]], axis=0)
        return jnp.dot(lhs, keys, preferred_element_type=jnp.float32)

    def masked(pair, s):
        b0 = 2 * pair
        s = s * HD ** (-0.5)
        parts = []
        for j in range(blocks):
            lim = [jnp.minimum(val_s[j, b0 + r], len_s[b0 + r] - base - j * BLK) for r in range(2)]
            limit = jnp.where(upper, lim[0], lim[1])
            parts.append(jnp.where(lane2 < limit, s[:, j * BLK : (j + 1) * BLK], NEG))
        return parts

    def tree(op, parts):
        while len(parts) > 1:
            parts = [op(parts[i], parts[i + 1]) for i in range(0, len(parts), 2)]
        return parts[0]

    def products(k):
        await_slots(qbuf, len(peers_of(k)), qrecv.at[k])
        return [product_of(pair) for pair in pairs_of(k)]

    def weigh(k, raw, carry):
        l0, l1, m0, m1 = carry
        pairs = pairs_of(k)
        parts = [masked(pair, s) for pair, s in zip(pairs, raw)]
        tops = [
            jnp.maximum(jnp.max(tree(jnp.maximum, ps), axis=1, keepdims=True), FLOOR) for ps in parts
        ]
        expos = [[jnp.exp(s - top) for s in ps] for ps, top in zip(parts, tops)]
        totals = [
            jnp.maximum(jnp.sum(tree(jnp.add, es), axis=1, keepdims=True), TINY) for es in expos
        ]
        weights = []
        for pair, top, es, total in zip(pairs, tops, expos, totals):
            w = jnp.concatenate(es, axis=1).astype(jnp.bfloat16)
            weights.append(w)
            pbuf[pl.ds(pl.multiple_of(pair * 2 * heads, 2 * heads), 2 * heads), :] = w
            ibuf[pair] = jnp.broadcast_to(1.0 / total, (2 * heads, HD))
            lse = top + jnp.log(total)
            for r in range(2):
                rows = slice(r * heads, (r + 1) * heads)
                at = (2 * pair + r) * heads
                l0 = jnp.where(skew == at, lse[rows], l0)
                l1 = jnp.where(skew == at - BLK, lse[rows], l1)
                m0 = jnp.where(skew == at, top[rows], m0)
                m1 = jnp.where(skew == at - BLK, top[rows], m1)
        return (l0, l1, m0, m1), weights

    def mixed_of(pair, w):
        vals = jnp.concatenate([vbuf[2 * pair], vbuf[2 * pair + 1]], axis=1)
        return jnp.dot(w, vals, preferred_element_type=jnp.float32)

    def keep(pair, mixed):
        inv = ibuf[pair]
        for r in range(2):
            rows = slice(r * heads, (r + 1) * heads)
            obuf[2 * pair + r] = (mixed[rows, r * HD : (r + 1) * HD] * inv[rows]).astype(jnp.bfloat16)

    def mix(k):
        for pair in pairs_of(k):
            keep(pair, mixed_of(pair, pbuf[pl.ds(pl.multiple_of(pair * 2 * heads, 2 * heads), 2 * heads), :]))

    zero = jnp.zeros((heads, BLK), jnp.float32)
    carry = (zero, zero, zero, zero)
    raw = products(0)
    for k in range(1, groups):
        later = products(k)
        carry, _ = weigh(k - 1, raw, carry)
        raw = later
    last = groups - 1
    (l0, l1, m0, m1), weights = weigh(last, raw, carry)
    mixed = [mixed_of(pair, w) for pair, w in zip(pairs_of(last), weights)]

    own = jnp.concatenate([jnp.sum(l0, axis=0, keepdims=True), jnp.sum(l1, axis=0, keepdims=True)], axis=0)
    tops = jnp.concatenate([jnp.sum(m0, axis=0, keepdims=True), jnp.sum(m1, axis=0, keepdims=True)], axis=0)
    stat[...] = own
    statall[me] = own

    for peer in peers_of(last):
        s_copy(peer).start()
    for pair, product in zip(pairs_of(last), mixed):
        keep(pair, product)
    for peer in peers_of(last):
        o_copy(peer).start()
    for k in far_first[1:]:
        for peer in peers_of(k):
            s_copy(peer).start()
    for k in far_first[1:]:
        mix(k)
        if k + 1 < last:
            for peer in peers_of(k + 1):
                o_copy(peer).start()
    mixbuf[me] = obuf[me]
    for peer in peers_of(0):
        o_copy(peer).start()
    await_slots(statall, n - 1, srecv)

    every = statall[...]
    top = jnp.max(every, axis=0)
    lse = top + jnp.log(jnp.sum(jnp.exp(every - top[None]), axis=0))
    ltot[...] = lse
    share = jnp.exp(tops - lse)
    rows_h = lax.broadcasted_iota(jnp.int32, (half, BLK), 0)
    lanes_h = lax.broadcasted_iota(jnp.int32, (half, BLK), 1) // heads
    for r in range(2):
        spread = jnp.where(rows_h == lanes_h, jnp.broadcast_to(share[r : r + 1], (half, BLK)), 0.0)
        high = spread.astype(jnp.bfloat16)
        low = (spread - high.astype(jnp.float32)).astype(jnp.bfloat16)
        both = jnp.concatenate([high, low], axis=0)
        got = jnp.dot(both, pbuf[r * BLK : (r + 1) * BLK, :], preferred_element_type=jnp.float32)
        got = got[:half] + got[half:]
        for j in range(blocks):
            at = pl.ds(r * half * blocks + j, half, stride=blocks)
            new_ref[at, :] = old_v[at, :] + got[:, j * BLK : (j + 1) * BLK]

    my_row = me // half
    hit = skew == (me % half) * heads
    total_row = ltot[pl.ds(my_row, 1), :]
    factors = []
    for d in range(n):
        gap = jnp.broadcast_to(statall[d, pl.ds(my_row, 1), :] - total_row, (heads, BLK))
        factors.append(jnp.exp(jnp.sum(jnp.where(hit, gap, 0.0), axis=1, keepdims=True)))
    await_slots(mixbuf, n - 1, orecv)
    acc = zero
    for d in range(n):
        acc = acc + factors[d] * mixbuf[d].astype(jnp.float32)
    att_ref[...] = acc

    both = kbuf.at[0, pl.ds(0, 2 * (n - 1) * heads)]
    pltpu.make_async_copy(both, both, osem).wait()
    await_slots(statall, n - 1, ssend)


def closing(new_ref, att_ref, heavy_ref, attended_ref):
    heavy_ref[...] = new_ref[...]
    attended_ref[...] = att_ref[...].astype(jnp.bfloat16)


def on_device(queries, keys, values, old_scores, lengths, valid_counts):
    n = lax.axis_size("seq")
    heads = queries.shape[1]
    ctx = keys.shape[2]
    blocks = ctx // BLK
    anywhere = pl.BlockSpec(memory_space=pltpu.HBM)
    vmem = pl.BlockSpec(memory_space=pltpu.VMEM)
    dma = pltpu.SemaphoreType.DMA
    updated, mixed = pl.pallas_call(
        functools.partial(kernel, n, heads, ctx),
        out_shape=(
            jax.ShapeDtypeStruct((n * blocks, BLK), jnp.float32),
            jax.ShapeDtypeStruct((heads, HD), jnp.float32),
        ),
        in_specs=[anywhere] * 6,
        out_specs=(vmem, vmem),
        scratch_shapes=[
            pltpu.VMEM((2, n, ctx, HD), jnp.bfloat16),
            pltpu.VMEM((n * blocks, BLK), jnp.float32),
            pltpu.VMEM((n, HD, ctx), jnp.bfloat16),
            pltpu.VMEM((n, heads, HD), jnp.bfloat16),
            pltpu.VMEM((n, heads, HD), jnp.bfloat16),
            pltpu.VMEM((n, heads, HD), jnp.bfloat16),
            pltpu.VMEM((n * heads, ctx), jnp.bfloat16),
            pltpu.VMEM((n // 2, 2 * heads, HD), jnp.float32),
            pltpu.VMEM((2, BLK), jnp.float32),
            pltpu.VMEM((n, 2, BLK), jnp.float32),
            pltpu.VMEM((2, BLK), jnp.float32),
            pltpu.SMEM((n,), jnp.int32),
            pltpu.SMEM((blocks, n), jnp.int32),
            dma,
            dma((4,)),
            dma,
            dma((NZ // 2,)),
            dma,
            dma,
            dma,
        ],
        compiler_params=pltpu.CompilerParams(
            collective_id=0, has_side_effects=True, vmem_limit_bytes=16 * 2**20
        ),
        name="decode",
    )(
        *(
            pltpu.with_memory_space_constraint(a, pltpu.HBM)
            for a in (queries, keys, values, old_scores.reshape(n * blocks, BLK), lengths, valid_counts.T)
        )
    )
    heavy, attended = pl.pallas_call(
        closing,
        out_shape=(
            jax.ShapeDtypeStruct((n * blocks, BLK), jnp.float32),
            jax.ShapeDtypeStruct((heads, HD), jnp.bfloat16),
        ),
        in_specs=[vmem] * 2,
        out_specs=(vmem, vmem),
        compiler_params=pltpu.CompilerParams(vmem_limit_bytes=2**20),
        name="closing",
    )(updated, mixed)
    return attended[None], heavy.reshape(old_scores.shape)


def solution(mesh):
    return jax.shard_map(
        on_device,
        mesh=mesh,
        in_specs=(
            P("seq", "head", None),
            P(None, "head", "seq", None),
            P(None, "head", "seq", None),
            P(None, "head", "seq"),
            P(),
            P(None, "seq"),
        ),
        out_specs=(P("seq", "head", None), P(None, "head", "seq")),
        check_vma=False,
    )
```

```python
import functools

import jax
import jax.numpy as jnp
from jax import lax
from jax.experimental import pallas as pl
from jax.experimental.pallas import tpu as pltpu
from jax.sharding import PartitionSpec as P

HD = 128
BLK = 128
NX, NZ = 4, 8
NEG = -1e30
FLOOR = -1e29
TINY = 1e-30
MESH = pl.DeviceIdType.MESH


def kernel(
    n, heads, ctx, q_hbm, k_hbm, v_hbm, old_hbm, len_hbm, val_hbm, new_ref, att_ref,
    kvbuf, old_v, kturn, qbuf, obuf, mixbuf, spare, pbuf, ibuf, stat, statall, ltot, len_s, val_s,
    kvsem, lsem, osem, qrecv, orecv, ssend, srecv,
):
    me = lax.axis_index("seq")
    mx, mz = me // NZ, me % NZ
    blocks = ctx // BLK
    half = n // 2

    places = NZ // 2
    mzo = mz // 2

    def pairs_of(zo):
        return [((mx + xo) % NX) * places + zo for xo in (2, 1, 3, 0)]

    def for_peers(zo, act, act_far=None):
        for i, pair in enumerate(pairs_of(zo)):
            for b in (2 * pair, 2 * pair + 1):
                if i == 0 and act_far is not None:
                    act_far(b)
                elif i < NX - 1:
                    act(b)
                else:
                    pl.when(b != me)(functools.partial(act, b))

    barrier = pltpu.get_barrier_semaphore()

    def greet(peer):
        pl.semaphore_signal(barrier, inc=1, device_id={"seq": peer}, device_id_type=MESH)

    for zo in range(places):
        for_peers(zo, greet)

    q_load = pltpu.make_async_copy(q_hbm.at[0], qbuf.at[me], lsem.at[0])
    len_load = pltpu.make_async_copy(len_hbm, len_s, lsem.at[1])
    val_load = pltpu.make_async_copy(val_hbm, val_s, lsem.at[2])
    q_load.start()
    pltpu.make_async_copy(q_hbm.at[0], spare, qrecv.at[mzo]).start()
    len_load.start()
    val_load.start()
    kbuf, vbuf = kvbuf.at[0], kvbuf.at[1]
    loads = [pltpu.make_async_copy(old_hbm, old_v, lsem.at[3])]
    for c in range(4):
        rows = pl.ds(c * (n // 4), n // 4)
        loads.append(pltpu.make_async_copy(k_hbm.at[rows, 0], kbuf.at[rows], kvsem))
        loads.append(pltpu.make_async_copy(v_hbm.at[rows, 0], vbuf.at[rows], kvsem))
    for load in loads:
        load.start()
    q_load.wait()
    pl.semaphore_wait(barrier, n - 1)

    far_sem = mzo + places * (1 - (mzo + places - 1) // places)

    def send_q(sem, peer):
        pltpu.make_async_remote_copy(
            src_ref=qbuf.at[me], dst_ref=qbuf.at[me], send_sem=osem, recv_sem=qrecv.at[sem],
            device_id={"seq": peer}, device_id_type=MESH,
        ).start()

    def send_o(b):
        pltpu.make_async_remote_copy(
            src_ref=obuf.at[b], dst_ref=mixbuf.at[me], send_sem=osem, recv_sem=orecv,
            device_id={"seq": b}, device_id_type=MESH,
        ).start()

    def send_s(peer):
        pltpu.make_async_remote_copy(
            src_ref=stat, dst_ref=statall.at[me], send_sem=ssend, recv_sem=srecv,
            device_id={"seq": peer}, device_id_type=MESH,
        ).start()

    def await_slots(buf, count, sem):
        some = buf.at[pl.ds(0, count)]
        pltpu.make_async_copy(some, some, sem).wait()

    for zo in (2, 3, 1, 0):
        for_peers(zo, functools.partial(send_q, mzo), functools.partial(send_q, far_sem))
    len_load.wait()
    val_load.wait()
    loads[0].wait()
    pltpu.make_async_copy(kvbuf, kvbuf, kvsem).wait()

    def turn(b, _):
        kturn[b] = kbuf[b].T
        return 0

    lax.fori_loop(0, n, turn, 0, unroll=4)

    base = me * ctx
    row2 = lax.broadcasted_iota(jnp.int32, (2 * heads, BLK), 0)
    lane2 = lax.broadcasted_iota(jnp.int32, (2 * heads, BLK), 1)
    upper = row2 < heads
    skew = (
        lax.broadcasted_iota(jnp.int32, (heads, BLK), 1)
        - lax.broadcasted_iota(jnp.int32, (heads, BLK), 0)
    )

    def product_of(pair):
        b0 = 2 * pair
        qp = qbuf[pl.ds(b0, 2)].astype(jnp.float32).reshape(2 * heads, HD)
        lhs = jnp.concatenate([jnp.where(upper, qp, 0.0), jnp.where(upper, 0.0, qp)], axis=1).astype(jnp.bfloat16)
        keys = jnp.concatenate([kturn[b0], kturn[b0 + 1]], axis=0)
        return jnp.dot(lhs, keys, preferred_element_type=jnp.float32)

    def masked(pair, s):
        b0 = 2 * pair
        s = s * HD ** (-0.5)
        parts = []
        for j in range(blocks):
            lim = [jnp.minimum(val_s[j, b0 + r], len_s[b0 + r] - base - j * BLK) for r in range(2)]
            limit = jnp.where(upper, lim[0], lim[1])
            parts.append(jnp.where(lane2 < limit, s[:, j * BLK : (j + 1) * BLK], NEG))
        return parts

    def tree(op, parts):
        while len(parts) > 1:
            parts = [op(parts[i], parts[i + 1]) for i in range(0, len(parts), 2)]
        return parts[0]

    def products(k, some=slice(None)):
        pairs = pairs_of(k)[some]
        at = places if k == 0 and some == slice(0, 1) else k
        await_slots(qbuf, 2 * len(pairs), qrecv.at[at])
        return [product_of(pair) for pair in pairs]

    def weigh(pairs, raw, carry):
        l0, l1, m0, m1 = carry
        parts = [masked(pair, s) for pair, s in zip(pairs, raw)]
        tops = [
            jnp.maximum(jnp.max(tree(jnp.maximum, ps), axis=1, keepdims=True), FLOOR) for ps in parts
        ]
        expos = [[jnp.exp(s - top) for s in ps] for ps, top in zip(parts, tops)]
        totals = [
            jnp.maximum(jnp.sum(tree(jnp.add, es), axis=1, keepdims=True), TINY) for es in expos
        ]
        weights = []
        for pair, top, es, total in zip(pairs, tops, expos, totals):
            w = jnp.concatenate(es, axis=1).astype(jnp.bfloat16)
            weights.append(w)
            pbuf[pl.ds(pl.multiple_of(pair * 2 * heads, 2 * heads), 2 * heads), :] = w
            ibuf[pair] = jnp.broadcast_to(1.0 / total, (2 * heads, HD))
            lse = top + jnp.log(total)
            for r in range(2):
                rows = slice(r * heads, (r + 1) * heads)
                at = (2 * pair + r) * heads
                l0 = jnp.where(skew == at, lse[rows], l0)
                l1 = jnp.where(skew == at - BLK, lse[rows], l1)
                m0 = jnp.where(skew == at, top[rows], m0)
                m1 = jnp.where(skew == at - BLK, top[rows], m1)
        return (l0, l1, m0, m1), weights

    def mixed_of(pair, w):
        vals = jnp.concatenate([vbuf[2 * pair], vbuf[2 * pair + 1]], axis=1)
        return jnp.dot(w, vals, preferred_element_type=jnp.float32)

    def keep(pair, mixed):
        inv = ibuf[pair]
        for r in range(2):
            rows = slice(r * heads, (r + 1) * heads)
            obuf[2 * pair + r] = (mixed[rows, r * HD : (r + 1) * HD] * inv[rows]).astype(jnp.bfloat16)

    def mix(k):
        for pair in pairs_of(k):
            keep(pair, mixed_of(pair, pbuf[pl.ds(pl.multiple_of(pair * 2 * heads, 2 * heads), 2 * heads), :]))

    zero = jnp.zeros((heads, BLK), jnp.float32)
    carry = (zero, zero, zero, zero)
    order = [(k, slice(None)) for k in range(places)[:0:-1]] + [(0, slice(1, None)), (0, slice(0, 1))]
    raw = products(*order[0])
    kept = []
    for (before, some), now in zip(order, order[1:]):
        later = products(*now)
        carry, kept = weigh(pairs_of(before)[some], raw, carry)
        raw = later
    (l0, l1, m0, m1), weights = weigh(pairs_of(0)[:1], raw, carry)
    weights = weights + kept
    mixed = [mixed_of(pair, w) for pair, w in zip(pairs_of(0), weights)]

    own = jnp.concatenate([jnp.sum(l0, axis=0, keepdims=True), jnp.sum(l1, axis=0, keepdims=True)], axis=0)
    tops = jnp.concatenate([jnp.sum(m0, axis=0, keepdims=True), jnp.sum(m1, axis=0, keepdims=True)], axis=0)
    stat[...] = own
    statall[me] = own

    for_peers(0, send_s)
    for pair, product in zip(pairs_of(0), mixed):
        keep(pair, product)
    for_peers(0, send_o)
    for_peers(1, send_s)
    mix(1)
    for_peers(1, send_o)
    for_peers(2, send_s)
    for_peers(3, send_s)
    for zo in (2, 3):
        mix(zo)
        for_peers(zo, send_o)
    mixbuf[me] = obuf[me]
    await_slots(statall, n - 1, srecv)

    every = statall[...]
    top = jnp.max(every, axis=0)
    lse = top + jnp.log(jnp.sum(jnp.exp(every - top[None]), axis=0))
    ltot[...] = lse
    share = jnp.exp(tops - lse)
    rows_h = lax.broadcasted_iota(jnp.int32, (half, BLK), 0)
    lanes_h = lax.broadcasted_iota(jnp.int32, (half, BLK), 1) // heads
    for r in range(2):
        spread = jnp.where(rows_h == lanes_h, jnp.broadcast_to(share[r : r + 1], (half, BLK)), 0.0)
        high = spread.astype(jnp.bfloat16)
        low = (spread - high.astype(jnp.float32)).astype(jnp.bfloat16)
        both = jnp.concatenate([high, low], axis=0)
        got = jnp.dot(both, pbuf[r * BLK : (r + 1) * BLK, :], preferred_element_type=jnp.float32)
        got = got[:half] + got[half:]
        for j in range(blocks):
            at = pl.ds(r * half * blocks + j, half, stride=blocks)
            new_ref[at, :] = old_v[at, :] + got[:, j * BLK : (j + 1) * BLK]

    my_row = me // half
    hit = skew == (me % half) * heads
    total_row = ltot[pl.ds(my_row, 1), :]
    factors = []
    for d in range(n):
        gap = jnp.broadcast_to(statall[d, pl.ds(my_row, 1), :] - total_row, (heads, BLK))
        factors.append(jnp.exp(jnp.sum(jnp.where(hit, gap, 0.0), axis=1, keepdims=True)))
    await_slots(mixbuf, n - 1, orecv)
    acc = zero
    for d in range(n):
        acc = acc + factors[d] * mixbuf[d].astype(jnp.float32)
    att_ref[...] = acc

    both = kbuf.at[0, pl.ds(0, 2 * (n - 1) * heads)]
    pltpu.make_async_copy(both, both, osem).wait()
    await_slots(statall, n - 1, ssend)


def closing(new_ref, att_ref, heavy_ref, attended_ref):
    heavy_ref[...] = new_ref[...]
    attended_ref[...] = att_ref[...].astype(jnp.bfloat16)


def on_device(queries, keys, values, old_scores, lengths, valid_counts):
    n = lax.axis_size("seq")
    heads = queries.shape[1]
    ctx = keys.shape[2]
    blocks = ctx // BLK
    anywhere = pl.BlockSpec(memory_space=pltpu.HBM)
    vmem = pl.BlockSpec(memory_space=pltpu.VMEM)
    dma = pltpu.SemaphoreType.DMA
    updated, mixed = pl.pallas_call(
        functools.partial(kernel, n, heads, ctx),
        out_shape=(
            jax.ShapeDtypeStruct((n * blocks, BLK), jnp.float32),
            jax.ShapeDtypeStruct((heads, HD), jnp.float32),
        ),
        in_specs=[anywhere] * 6,
        out_specs=(vmem, vmem),
        scratch_shapes=[
            pltpu.VMEM((2, n, ctx, HD), jnp.bfloat16),
            pltpu.VMEM((n * blocks, BLK), jnp.float32),
            pltpu.VMEM((n, HD, ctx), jnp.bfloat16),
            pltpu.VMEM((n, heads, HD), jnp.bfloat16),
            pltpu.VMEM((n, heads, HD), jnp.bfloat16),
            pltpu.VMEM((n, heads, HD), jnp.bfloat16),
            pltpu.VMEM((heads, HD), jnp.bfloat16),
            pltpu.VMEM((n * heads, ctx), jnp.bfloat16),
            pltpu.VMEM((n // 2, 2 * heads, HD), jnp.float32),
            pltpu.VMEM((2, BLK), jnp.float32),
            pltpu.VMEM((n, 2, BLK), jnp.float32),
            pltpu.VMEM((2, BLK), jnp.float32),
            pltpu.SMEM((n,), jnp.int32),
            pltpu.SMEM((blocks, n), jnp.int32),
            dma,
            dma((4,)),
            dma,
            dma((NZ // 2 + 1,)),
            dma,
            dma,
            dma,
        ],
        compiler_params=pltpu.CompilerParams(
            collective_id=0, has_side_effects=True, vmem_limit_bytes=16 * 2**20
        ),
        name="decode",
    )(
        *(
            pltpu.with_memory_space_constraint(a, pltpu.HBM)
            for a in (queries, keys, values, old_scores.reshape(n * blocks, BLK), lengths, valid_counts.T)
        )
    )
    heavy, attended = pl.pallas_call(
        closing,
        out_shape=(
            jax.ShapeDtypeStruct((n * blocks, BLK), jnp.float32),
            jax.ShapeDtypeStruct((heads, HD), jnp.bfloat16),
        ),
        in_specs=[vmem] * 2,
        out_specs=(vmem, vmem),
        compiler_params=pltpu.CompilerParams(vmem_limit_bytes=2**20),
        name="closing",
    )(updated, mixed)
    return attended[None], heavy.reshape(old_scores.shape)


def solution(mesh):
    return jax.shard_map(
        on_device,
        mesh=mesh,
        in_specs=(
            P("seq", "head", None),
            P(None, "head", "seq", None),
            P(None, "head", "seq", None),
            P(None, "head", "seq"),
            P(),
            P(None, "seq"),
        ),
        out_specs=(P("seq", "head", None), P(None, "head", "seq")),
        check_vma=False,
    )
```

```python
import functools

import jax
import jax.numpy as jnp
from jax import lax
from jax.experimental import pallas as pl
from jax.experimental.pallas import tpu as pltpu
from jax.sharding import PartitionSpec as P

HD = 128
BLK = 128
NX, NZ = 4, 8
NEG = -1e30
FLOOR = -1e29
TINY = 1e-30
MESH = pl.DeviceIdType.MESH


def kernel(
    n, heads, ctx, q_hbm, k_hbm, v_hbm, old_hbm, len_hbm, val_hbm, new_ref, att_ref,
    kvbuf, old_v, kturn, qbuf, obuf, mixbuf, spare, pbuf, ibuf, stat, statall, ltot, len_s, val_s,
    kvsem, lsem, qsend, osem, qrecv, orecv, ssend, srecv,
):
    me = lax.axis_index("seq")
    mx, mz = me // NZ, me % NZ
    blocks = ctx // BLK
    half = n // 2

    places = NZ // 2
    mzo = mz // 2

    def pairs_of(zo):
        return [((mx + xo) % NX) * places + zo for xo in (2, 1, 3, 0)]

    def for_peers(zo, act, act_far=None):
        for i, pair in enumerate(pairs_of(zo)):
            for b in (2 * pair, 2 * pair + 1):
                if i == 0 and act_far is not None:
                    act_far(b)
                elif i < NX - 1:
                    act(b)
                else:
                    pl.when(b != me)(functools.partial(act, b))

    barrier = pltpu.get_barrier_semaphore()

    def greet(peer):
        pl.semaphore_signal(barrier, inc=1, device_id={"seq": peer}, device_id_type=MESH)

    for zo in range(places):
        for_peers(zo, greet)

    q_load = pltpu.make_async_copy(q_hbm.at[0], qbuf.at[me], lsem.at[0])
    len_load = pltpu.make_async_copy(len_hbm, len_s, lsem.at[1])
    val_load = pltpu.make_async_copy(val_hbm, val_s, lsem.at[2])
    q_load.start()
    pltpu.make_async_copy(q_hbm.at[0], spare, qrecv.at[mzo]).start()
    len_load.start()
    val_load.start()
    kbuf, vbuf = kvbuf.at[0], kvbuf.at[1]
    loads = [pltpu.make_async_copy(old_hbm, old_v, lsem.at[3])]
    for c in range(4):
        rows = pl.ds(c * (n // 4), n // 4)
        loads.append(pltpu.make_async_copy(k_hbm.at[rows, 0], kbuf.at[rows], kvsem))
        loads.append(pltpu.make_async_copy(v_hbm.at[rows, 0], vbuf.at[rows], kvsem))
    for load in loads:
        load.start()
    q_load.wait()
    pl.semaphore_wait(barrier, n - 1)

    far_sem = mzo + places * (1 - (mzo + places - 1) // places)

    def send_q(sem, peer):
        pltpu.make_async_remote_copy(
            src_ref=qbuf.at[me], dst_ref=qbuf.at[me], send_sem=qsend, recv_sem=qrecv.at[sem],
            device_id={"seq": peer}, device_id_type=MESH,
        ).start()

    def send_o(b):
        pltpu.make_async_remote_copy(
            src_ref=obuf.at[b], dst_ref=mixbuf.at[me], send_sem=osem, recv_sem=orecv,
            device_id={"seq": b}, device_id_type=MESH,
        ).start()

    def send_s(peer):
        pltpu.make_async_remote_copy(
            src_ref=stat, dst_ref=statall.at[me], send_sem=ssend, recv_sem=srecv,
            device_id={"seq": peer}, device_id_type=MESH,
        ).start()

    def await_slots(buf, count, sem):
        some = buf.at[pl.ds(0, count)]
        pltpu.make_async_copy(some, some, sem).wait()

    for zo in (2, 3, 1, 0):
        for_peers(zo, functools.partial(send_q, mzo), functools.partial(send_q, far_sem))
    len_load.wait()
    val_load.wait()
    loads[0].wait()
    pltpu.make_async_copy(kvbuf, kvbuf, kvsem).wait()

    def turn(b, _):
        kturn[b] = kbuf[b].T
        return 0

    lax.fori_loop(0, n, turn, 0, unroll=4)

    base = me * ctx
    row2 = lax.broadcasted_iota(jnp.int32, (2 * heads, BLK), 0)
    lane2 = lax.broadcasted_iota(jnp.int32, (2 * heads, BLK), 1)
    upper = row2 < heads
    skew = (
        lax.broadcasted_iota(jnp.int32, (heads, BLK), 1)
        - lax.broadcasted_iota(jnp.int32, (heads, BLK), 0)
    )

    def product_of(pair):
        b0 = 2 * pair
        qp = qbuf[pl.ds(b0, 2)].astype(jnp.float32).reshape(2 * heads, HD)
        lhs = jnp.concatenate([jnp.where(upper, qp, 0.0), jnp.where(upper, 0.0, qp)], axis=1).astype(jnp.bfloat16)
        keys = jnp.concatenate([kturn[b0], kturn[b0 + 1]], axis=0)
        return jnp.dot(lhs, keys, preferred_element_type=jnp.float32)

    def masked(pair, s):
        b0 = 2 * pair
        s = s * HD ** (-0.5)
        parts = []
        for j in range(blocks):
            lim = [jnp.minimum(val_s[j, b0 + r], len_s[b0 + r] - base - j * BLK) for r in range(2)]
            limit = jnp.where(upper, lim[0], lim[1])
            parts.append(jnp.where(lane2 < limit, s[:, j * BLK : (j + 1) * BLK], NEG))
        return parts

    def tree(op, parts):
        while len(parts) > 1:
            parts = [op(parts[i], parts[i + 1]) for i in range(0, len(parts), 2)]
        return parts[0]

    def products(k, some=slice(None)):
        pairs = pairs_of(k)[some]
        at = places if k == 0 and some == slice(0, 1) else k
        await_slots(qbuf, 2 * len(pairs), qrecv.at[at])
        return [product_of(pair) for pair in pairs]

    def weigh(pairs, raw, carry):
        l0, l1, m0, m1 = carry
        parts = [masked(pair, s) for pair, s in zip(pairs, raw)]
        tops = [
            jnp.maximum(jnp.max(tree(jnp.maximum, ps), axis=1, keepdims=True), FLOOR) for ps in parts
        ]
        expos = [[jnp.exp(s - top) for s in ps] for ps, top in zip(parts, tops)]
        totals = [
            jnp.maximum(jnp.sum(tree(jnp.add, es), axis=1, keepdims=True), TINY) for es in expos
        ]
        weights = []
        for pair, top, es, total in zip(pairs, tops, expos, totals):
            w = jnp.concatenate(es, axis=1).astype(jnp.bfloat16)
            weights.append(w)
            pbuf[pl.ds(pl.multiple_of(pair * 2 * heads, 2 * heads), 2 * heads), :] = w
            ibuf[pair] = jnp.broadcast_to(1.0 / total, (2 * heads, HD))
            lse = top + jnp.log(total)
            for r in range(2):
                rows = slice(r * heads, (r + 1) * heads)
                at = (2 * pair + r) * heads
                l0 = jnp.where(skew == at, lse[rows], l0)
                l1 = jnp.where(skew == at - BLK, lse[rows], l1)
                m0 = jnp.where(skew == at, top[rows], m0)
                m1 = jnp.where(skew == at - BLK, top[rows], m1)
        return (l0, l1, m0, m1), weights

    def mixed_of(pair, w):
        vals = jnp.concatenate([vbuf[2 * pair], vbuf[2 * pair + 1]], axis=1)
        return jnp.dot(w, vals, preferred_element_type=jnp.float32)

    def keep(pair, mixed):
        inv = ibuf[pair]
        for r in range(2):
            rows = slice(r * heads, (r + 1) * heads)
            obuf[2 * pair + r] = mixed[rows, r * HD : (r + 1) * HD] * inv[rows]

    def mix(k):
        for pair in pairs_of(k):
            keep(pair, mixed_of(pair, pbuf[pl.ds(pl.multiple_of(pair * 2 * heads, 2 * heads), 2 * heads), :]))

    zero = jnp.zeros((heads, BLK), jnp.float32)
    carry = (zero, zero, zero, zero)
    order = [(k, slice(None)) for k in range(places)[:0:-1]] + [(0, slice(1, None)), (0, slice(0, 1))]
    raw = products(*order[0])
    kept = []
    for (before, some), now in zip(order, order[1:]):
        later = products(*now)
        carry, kept = weigh(pairs_of(before)[some], raw, carry)
        raw = later
    (l0, l1, m0, m1), weights = weigh(pairs_of(0)[:1], raw, carry)
    weights = weights + kept
    mixed = [mixed_of(pair, w) for pair, w in zip(pairs_of(0), weights)]

    own = jnp.concatenate([jnp.sum(l0, axis=0, keepdims=True), jnp.sum(l1, axis=0, keepdims=True)], axis=0)
    tops = jnp.concatenate([jnp.sum(m0, axis=0, keepdims=True), jnp.sum(m1, axis=0, keepdims=True)], axis=0)
    stat[...] = own
    statall[me] = own

    for_peers(0, send_s)
    for pair, product in zip(pairs_of(0), mixed):
        keep(pair, product)
    for_peers(0, send_o)
    for_peers(1, send_s)
    mix(1)
    for_peers(1, send_o)
    for_peers(2, send_s)
    for_peers(3, send_s)
    for zo in (2, 3):
        mix(zo)
        for_peers(zo, send_o)
    mixbuf[me] = obuf[me]
    await_slots(statall, n - 1, srecv)

    every = statall[...]
    top = jnp.max(every, axis=0)
    lse = top + jnp.log(jnp.sum(jnp.exp(every - top[None]), axis=0))
    ltot[...] = lse
    share = jnp.exp(tops - lse)
    rows_h = lax.broadcasted_iota(jnp.int32, (half, BLK), 0)
    lanes_h = lax.broadcasted_iota(jnp.int32, (half, BLK), 1) // heads
    for r in range(2):
        spread = jnp.where(rows_h == lanes_h, jnp.broadcast_to(share[r : r + 1], (half, BLK)), 0.0)
        high = spread.astype(jnp.bfloat16)
        low = (spread - high.astype(jnp.float32)).astype(jnp.bfloat16)
        both = jnp.concatenate([high, low], axis=0)
        got = jnp.dot(both, pbuf[r * BLK : (r + 1) * BLK, :], preferred_element_type=jnp.float32)
        got = got[:half] + got[half:]
        for j in range(blocks):
            at = pl.ds(r * half * blocks + j, half, stride=blocks)
            new_ref[at, :] = old_v[at, :] + got[:, j * BLK : (j + 1) * BLK]

    my_row = me // half
    hit = skew == (me % half) * heads
    total_row = ltot[pl.ds(my_row, 1), :]
    factors = []
    for d in range(n):
        gap = jnp.broadcast_to(statall[d, pl.ds(my_row, 1), :] - total_row, (heads, BLK))
        factors.append(jnp.exp(jnp.sum(jnp.where(hit, gap, 0.0), axis=1, keepdims=True)))
    await_slots(mixbuf, n - 1, orecv)
    acc = zero
    for d in range(n):
        acc = acc + factors[d] * mixbuf[d]
    att_ref[...] = acc

    await_slots(qbuf, n - 1, qsend)
    await_slots(obuf, n - 1, osem)
    await_slots(statall, n - 1, ssend)


def closing(new_ref, att_ref, heavy_ref, attended_ref):
    heavy_ref[...] = new_ref[...]
    attended_ref[...] = att_ref[...].astype(jnp.bfloat16)


def on_device(queries, keys, values, old_scores, lengths, valid_counts):
    n = lax.axis_size("seq")
    heads = queries.shape[1]
    ctx = keys.shape[2]
    blocks = ctx // BLK
    anywhere = pl.BlockSpec(memory_space=pltpu.HBM)
    vmem = pl.BlockSpec(memory_space=pltpu.VMEM)
    dma = pltpu.SemaphoreType.DMA
    updated, mixed = pl.pallas_call(
        functools.partial(kernel, n, heads, ctx),
        out_shape=(
            jax.ShapeDtypeStruct((n * blocks, BLK), jnp.float32),
            jax.ShapeDtypeStruct((heads, HD), jnp.float32),
        ),
        in_specs=[anywhere] * 6,
        out_specs=(vmem, vmem),
        scratch_shapes=[
            pltpu.VMEM((2, n, ctx, HD), jnp.bfloat16),
            pltpu.VMEM((n * blocks, BLK), jnp.float32),
            pltpu.VMEM((n, HD, ctx), jnp.bfloat16),
            pltpu.VMEM((n, heads, HD), jnp.bfloat16),
            pltpu.VMEM((n, heads, HD), jnp.float32),
            pltpu.VMEM((n, heads, HD), jnp.float32),
            pltpu.VMEM((heads, HD), jnp.bfloat16),
            pltpu.VMEM((n * heads, ctx), jnp.bfloat16),
            pltpu.VMEM((n // 2, 2 * heads, HD), jnp.float32),
            pltpu.VMEM((2, BLK), jnp.float32),
            pltpu.VMEM((n, 2, BLK), jnp.float32),
            pltpu.VMEM((2, BLK), jnp.float32),
            pltpu.SMEM((n,), jnp.int32),
            pltpu.SMEM((blocks, n), jnp.int32),
            dma,
            dma((4,)),
            dma,
            dma,
            dma((NZ // 2 + 1,)),
            dma,
            dma,
            dma,
        ],
        compiler_params=pltpu.CompilerParams(
            collective_id=0, has_side_effects=True, vmem_limit_bytes=16 * 2**20
        ),
        name="decode",
    )(
        *(
            pltpu.with_memory_space_constraint(a, pltpu.HBM)
            for a in (queries, keys, values, old_scores.reshape(n * blocks, BLK), lengths, valid_counts.T)
        )
    )
    heavy, attended = pl.pallas_call(
        closing,
        out_shape=(
            jax.ShapeDtypeStruct((n * blocks, BLK), jnp.float32),
            jax.ShapeDtypeStruct((heads, HD), jnp.bfloat16),
        ),
        in_specs=[vmem] * 2,
        out_specs=(vmem, vmem),
        compiler_params=pltpu.CompilerParams(vmem_limit_bytes=2**20),
        name="closing",
    )(updated, mixed)
    return attended[None], heavy.reshape(old_scores.shape)


def solution(mesh):
    return jax.shard_map(
        on_device,
        mesh=mesh,
        in_specs=(
            P("seq", "head", None),
            P(None, "head", "seq", None),
            P(None, "head", "seq", None),
            P(None, "head", "seq"),
            P(),
            P(None, "seq"),
        ),
        out_specs=(P("seq", "head", None), P(None, "head", "seq")),
        check_vma=False,
    )
```
